1024 devices in a mesh: pp: 8 (over z_lo, core), tp: 16 (over z_hi, x), dp: 8 (over y).
Axes of the slice: x: 4, y: 8, z: 16 (z_hi: 4, z_lo: 4; z = z_hi * 4 + z_lo), core: 2. Of those that a mesh axis runs over, the one named last changes fastest.
Arguments:
- act_in: bfloat16 [8, 8, 128, 4096], P('pp', 'dp', 'tp'), may hold values from -6 to 6
- stash_in: bfloat16 [8, 8, 128, 4096], P('pp', 'dp', 'tp'), may hold values from -6 to 6
- grad_in: bfloat16 [8, 8, 128, 4096], P('pp', 'dp', 'tp'), may hold values from -6 to 6
- doc_ids: int32 [8, 8, 2, 128], P('pp', 'dp'), may hold values from 0 to 15, never falling along the last dimension, each value on 1 to 64 neighbouring positions
- query_weight: bfloat16 [8, 4096, 4096], P('pp', None, 'tp'), as said below
- key_weight: bfloat16 [8, 4096, 2048], P('pp', None, 'tp'), as said below
- value_weight: bfloat16 [8, 4096, 2048], P('pp', None, 'tp'), as said below
- out_weight: bfloat16 [8, 4096, 4096], P('pp', None, 'tp'), may hold values from -0.09375 to 0.09375
Outputs:
- act_out: bfloat16 [8, 8, 128, 4096], P('pp', 'dp', 'tp')
- grad_out: bfloat16 [8, 8, 128, 4096], P('pp', 'dp', 'tp')
- grad_query: float32 [8, 4096, 4096], P('pp', 'dp', 'tp')
- grad_key: float32 [8, 4096, 2048], P('pp', 'dp', 'tp')
- grad_value: float32 [8, 4096, 2048], P('pp', 'dp', 'tp')
The draws below stay inside these ranges and needn't reach their ends.
Inputs may be any that keep to these rules, and one draw needn't show every extreme that they name: `doc_ids`: along each row of 128 positions the document numbers never fall. `query_weight`: entries of mean zero. `key_weight`: for each of the 8 key heads, its 2 stored copies (consecutive blocks of 128 columns) are equal; entries of mean zero. `value_weight`: for each of the 8 value heads, its 2 stored copies (consecutive blocks of 128 columns) are equal.
All inputs are finite; a program needn't handle non-finite values.
Results may differ from the reference program's by a relative error of at most 0.033.
Values may be sent and summed in bfloat16 or wider, within the bound.
No kernel may reach another device: no remote copies, remote signals or barrier semaphores. Data moves between devices by JAX's collectives and lax.ppermute only.
A program may use at most 64 MiB of HBM per device.

```python
import math
import jax
import jax.numpy as jnp
import numpy as np
from jax import lax

D = 4096
HEADS = 32
KV = 8
HEAD = 128
SEQ = 128
SPREAD = 2
N_PP = 8
N_TP = 16
N_DP = 8


def shared_heads(key, salt):
    base = jax.random.normal(jax.random.fold_in(key, salt), (N_PP, D, KV, 1, HEAD), jnp.float32)
    base = jnp.clip(base, -5.0, 5.0) / math.sqrt(D)
    return jnp.broadcast_to(base, (N_PP, D, KV, SPREAD, HEAD)).reshape(N_PP, D, KV * SPREAD, HEAD)


def draw_key_weight(key, part):
    return shared_heads(key, 11).reshape(N_PP, D, KV * SPREAD * HEAD).astype(jnp.bfloat16)


def draw_value_weight(key, part):
    return shared_heads(key, 13).reshape(N_PP, D, KV * SPREAD * HEAD).astype(jnp.bfloat16)


def draw_query_weight(key, part):
    fresh = jax.random.normal(jax.random.fold_in(key, 12), (N_PP, D, HEADS * HEAD), jnp.float32)
    fresh = jnp.clip(fresh, -5.0, 5.0) / math.sqrt(D)
    return fresh.astype(jnp.bfloat16)


def block_levels(key, dims, cuts, least, top_value):
    loudness = 1.0
    for axis_at, shards_of in cuts:
        heights = jax.random.uniform(jax.random.fold_in(jax.random.fold_in(key, 6), axis_at), (shards_of,), jnp.float32, least / len(cuts), top_value / len(cuts))
        loudness = loudness * jnp.repeat(jnp.exp(heights), dims[axis_at] // shards_of).reshape((-1,) + (1,) * (len(dims) - 1 - axis_at))
    return loudness


def profile(count, total, reach, skew):
    weights = [(1 << 20) // math.isqrt(grade ** skew) + 1 for grade in range(2, count + 1)]
    spare, given = total - reach - (count - 1), [1] * (count - 1)
    while spare > 0:
        movable = [i for i in range(count - 1) if given[i] < reach]
        whole, left = sum([weights[i] for i in movable]), spare
        for i in movable:
            addition = min(reach - given[i], max(1, left * weights[i] // whole), spare)
            given[i] = given[i] + addition
            spare = spare - addition
    return np.array([reach] + given)


def ragged_sizes(own_key, count, total, limit, slope):
    if count == 2:
        one = jax.random.randint(own_key, (), max(1, total - limit), min(limit, total - 1) + 1)
        return jnp.stack([one, total - one])
    lengths = jnp.asarray(profile(count, total, limit, slope), jnp.int32)
    twos = (count - 1) // 2
    giver, sink = lengths[1:1 + 2 * twos:2], lengths[2:2 + 2 * twos:2]
    room = jnp.minimum(giver - 1, limit - sink)
    passed = jax.random.randint(jax.random.fold_in(own_key, 1), (twos,), 0, 1 << 20) % (room + 1)
    lengths = lengths.at[1:1 + 2 * twos:2].set(giver - passed).at[2:2 + 2 * twos:2].set(sink + passed)
    return lengths[jax.random.permutation(jax.random.fold_in(own_key, 2), count)]


def noise(key, shape, deviation, limit, split=(), held_as=jnp.bfloat16):
    result = deviation * jax.random.normal(key, shape, jnp.float32)
    if split:
        result = result * block_levels(key, shape, split, -0.22, 0.18)
    return jnp.clip(result, -limit, limit).astype(held_as)


def setup_inputs(seed: int = 0) -> dict:
    streams_of = jax.random.split(jax.random.key(seed), 9)
    return {
        "act_in": noise(streams_of[0], (N_PP, N_DP, SEQ, D), 1.0, 6.0, ((0, 8), (1, 8), (2, 16))),
        "stash_in": noise(streams_of[1], (N_PP, N_DP, SEQ, D), 1.0, 6.0, ((0, 8), (1, 8), (2, 16))),
        "grad_in": noise(streams_of[2], (N_PP, N_DP, SEQ, D), 1.0, 6.0, ((0, 8), (1, 8), (2, 16))),
        "doc_ids": jax.vmap(lambda own: jnp.searchsorted(jnp.cumsum(ragged_sizes(own, SEQ // 8, SEQ, SEQ // 2, 2)), jnp.arange(SEQ), side="right"))(jax.random.split(streams_of[3], N_PP * N_DP * 2)).reshape((N_PP, N_DP, 2, SEQ)).astype(jnp.int32),
        "query_weight": draw_query_weight(jax.random.fold_in(streams_of[8], 71), 0),
        "key_weight": draw_key_weight(jax.random.fold_in(streams_of[8], 71), 0),
        "value_weight": draw_value_weight(jax.random.fold_in(streams_of[8], 71), 0),
        "out_weight": noise(streams_of[7], (N_PP, D, HEADS * HEAD), (HEADS * HEAD) ** -0.5, 0.09375, ((0, 8), (2, 16))),
    }


epsilon = 1e-05

def norm_rows(token_rows):
    widened = token_rows.astype(jnp.float32)
    inverse = lax.rsqrt(lax.optimization_barrier(jnp.mean(widened * widened, axis=-1, keepdims=True)) + epsilon)
    return ((widened * inverse).astype(jnp.bfloat16), inverse)

def allowed(documents):
    length = documents.shape[0]
    position = jnp.arange(length, dtype=jnp.int32)
    return (position[None, :] <= position[:, None]) & (documents[:, None] == documents[None, :])

def project(normed, weight):
    return jnp.dot(normed, weight, preferred_element_type=jnp.float32).astype(jnp.bfloat16)

def contract_first(left_side, right_side):
    return lax.dot_general(left_side, right_side, (((0,), (0,)), ((), ())), preferred_element_type=jnp.float32)

def split_heads(queries, keys, values):
    length = queries.shape[0]
    key_count = KV * SPREAD
    group_size = HEADS // key_count
    query_heads = queries.astype(jnp.float32).reshape(length, key_count, group_size, HEAD)
    key_heads = keys.astype(jnp.float32).reshape(length, key_count, HEAD)
    value_heads = values.astype(jnp.float32).reshape(length, key_count, HEAD)
    return (query_heads, key_heads, value_heads)

def attend(queries, keys, values, allowed_pairs):
    length = queries.shape[0]
    query_heads, key_heads, value_heads = split_heads(queries, keys, values)
    scores = jnp.einsum('ihgd,jhd->hgij', query_heads, key_heads) * (1.0 / math.sqrt(HEAD))
    scores = jnp.where(allowed_pairs, scores, -jnp.inf)
    row_max = lax.optimization_barrier(jnp.max(scores, axis=-1, keepdims=True))
    weights = jnp.exp(scores - row_max)
    probs = (weights / lax.optimization_barrier(jnp.sum(weights, axis=-1, keepdims=True))).astype(jnp.bfloat16)
    mixed = jnp.einsum('hgij,jhd->ihgd', probs.astype(jnp.float32), value_heads)
    return (probs, mixed.astype(jnp.bfloat16).reshape(length, HEADS * HEAD))

def attend_back(dmixed, queries, keys, values, probs):
    length = queries.shape[0]
    query_heads, key_heads, value_heads = split_heads(queries, keys, values)
    dmixed_heads = dmixed.astype(jnp.float32).reshape(query_heads.shape)
    dprobs = jnp.einsum('ihgd,jhd->hgij', dmixed_heads, value_heads)
    weights = probs.astype(jnp.float32)
    inner = lax.optimization_barrier(jnp.sum(weights * dprobs, axis=-1, keepdims=True))
    dscores = (weights * (dprobs - inner) * (1.0 / math.sqrt(HEAD))).astype(jnp.bfloat16)
    dqueries = jnp.einsum('hgij,jhd->ihgd', dscores.astype(jnp.float32), key_heads)
    dkeys = jnp.einsum('hgij,ihgd->jhd', dscores.astype(jnp.float32), query_heads)
    dvalues = jnp.einsum('hgij,ihgd->jhd', weights, dmixed_heads)
    return (dqueries.astype(jnp.bfloat16).reshape(length, HEADS * HEAD), dkeys.reshape(length, KV * SPREAD * HEAD), dvalues.reshape(length, KV * SPREAD * HEAD))

def rounded(product):
    return lax.optimization_barrier(product.astype(jnp.bfloat16)).astype(jnp.float32)

def group_sum(pairs):
    total = None
    for left_side, weight in pairs:
        length = left_side.shape[0]
        width = left_side.shape[1] // N_TP
        term = jnp.einsum('snc,dnc->nsd', left_side.astype(jnp.float32).reshape(length, N_TP, width), weight.astype(jnp.float32).reshape(weight.shape[0], N_TP, width))
        total = term if total is None else total + term
    return lax.optimization_barrier(jnp.sum(rounded(total), axis=0))

def section(inputs):
    forward_in, backward_in, incoming, documents, w_query, w_key, w_value, w_out = inputs

    def copy_step(totals, item):
        forward_rows, backward_rows, grad_rows, copy_docs = item
        normed_ahead, unused_inverse = norm_rows(forward_rows)
        probs_ahead, mixed_ahead = attend(project(normed_ahead, w_query), project(normed_ahead, w_key), project(normed_ahead, w_value), allowed(copy_docs[0]))
        attended = group_sum([(mixed_ahead, w_out)])
        outgoing = (forward_rows.astype(jnp.float32) + attended).astype(jnp.bfloat16)
        normed_back, inverse_back = norm_rows(backward_rows)
        queries = project(normed_back, w_query)
        keys = project(normed_back, w_key)
        values = project(normed_back, w_value)
        probs_back, unused_mixed = attend(queries, keys, values, allowed(copy_docs[1]))
        dmixed = jnp.dot(grad_rows, w_out, preferred_element_type=jnp.float32).astype(jnp.bfloat16)
        dqueries, dkeys, dvalues = attend_back(dmixed, queries, keys, values, probs_back)
        dkeys = dkeys.astype(jnp.bfloat16)
        dvalues = dvalues.astype(jnp.bfloat16)
        dnormed = group_sum([(dqueries, w_query), (dkeys, w_key), (dvalues, w_value)])
        scaled = backward_rows.astype(jnp.float32) * inverse_back
        grad_back = grad_rows.astype(jnp.float32) + inverse_back * (dnormed - scaled * lax.optimization_barrier(jnp.mean(dnormed * scaled, axis=-1, keepdims=True)))
        new_totals = (totals[0] + rounded(contract_first(normed_back, dqueries)), totals[1] + rounded(contract_first(normed_back, dkeys)), totals[2] + rounded(contract_first(normed_back, dvalues)))
        return (new_totals, (outgoing, grad_back.astype(jnp.bfloat16)))
    zeros = (jnp.zeros((D, HEADS * HEAD), jnp.float32), jnp.zeros((D, KV * SPREAD * HEAD), jnp.float32), jnp.zeros((D, KV * SPREAD * HEAD), jnp.float32))
    totals, (outgoing, grad_back) = lax.scan(copy_step, zeros, (forward_in, backward_in, incoming, documents))
    return (outgoing, grad_back, totals[0], totals[1], totals[2])

def reference(act_in, stash_in, grad_in, doc_ids, query_weight, key_weight, value_weight, out_weight):
    outgoing, grad_back, grad_query, grad_key, grad_value = lax.map(section, (act_in, stash_in, grad_in, doc_ids, query_weight, key_weight, value_weight, out_weight))
    act_out = jnp.roll(outgoing, 1, axis=0)
    grad_out = jnp.roll(grad_back, -1, axis=0)
    return (act_out, grad_out, grad_query, grad_key, grad_value)
```

```python
import math

import jax
import jax.numpy as jnp
from jax import lax
from jax.experimental import pallas as pl
from jax.experimental.pallas import tpu as pltpu
from jax.sharding import Mesh, PartitionSpec as P


HEAD = 128
SCALE = 1.0 / math.sqrt(HEAD)
STRIPE = 512
epsilon = 1e-05
bf16 = jnp.bfloat16
f32 = jnp.float32


def shift(value, axis, steps):
    count = lax.axis_size(axis)
    return lax.ppermute(value, axis, [(i, (i + steps) % count) for i in range(count)])


def swap(blocks, axis):
    return lax.all_to_all(blocks, axis, 0, 0, tiled=True)


def dot(a, b, left, right):
    return lax.dot_general(a, b, (((left,), (right,)), ((), ())), preferred_element_type=f32)


def nn(a, b):
    return dot(a, b, 1, 0)


def nt(a, b):
    return dot(a, b, 1, 1)


def tn(a, b):
    return dot(a, b, 0, 0)


def kernel(fn, out, scratch, *args, flops=0, room=16):
    vmem = pl.BlockSpec(memory_space=pltpu.VMEM)
    smem = pl.BlockSpec(memory_space=pltpu.SMEM)
    size = sum(a.size * a.dtype.itemsize for a in args)
    return pl.pallas_call(
        fn,
        out_shape=out,
        in_specs=[smem if a.shape == (1,) else vmem for a in args],
        out_specs=jax.tree.map(lambda _: vmem, out),
        scratch_shapes=scratch,
        compiler_params=pltpu.CompilerParams(vmem_limit_bytes=room << 20),
        cost_estimate=pl.CostEstimate(flops=flops, bytes_accessed=size, transcendentals=0),
    )(*args)


def struct(shape, dtype=bf16):
    return jax.ShapeDtypeStruct(shape, dtype)


def unit(rows):
    wide = rows.astype(f32)
    inverse = lax.rsqrt(jnp.mean(wide * wide, axis=-1, keepdims=True) + epsilon)
    return wide * inverse, inverse


def norm_body(stash, grad, act, out):
    width = act.shape[1]
    out[:, :width] = unit(stash[...])[0].astype(bf16)
    out[:, width : 2 * width] = grad[...]
    out[:, 2 * width :] = unit(act[...])[0].astype(bf16)


def bias_of(here, docs, share):
    seq = docs.shape[1]
    count = 4
    wide = seq // count

    def position(axis):
        row = lax.broadcasted_iota(jnp.int32, (seq, seq), axis)
        step = row // wide
        at_x = lax.rem(here + step, count)
        at_z = (row - step * wide) // share
        return (at_z * count + at_x) * share + lax.rem(row, share)

    pick = (lax.broadcasted_iota(jnp.int32, (seq, seq), 1) == position(0)).astype(f32)
    lined = jnp.broadcast_to(docs.astype(f32), (8, seq))
    down = nt(pick, lined)[:, :1]
    along = nt(lined, pick)[:1, :]
    return jnp.where((position(1) <= position(0)) & (down == along), 0.0, -jnp.inf).astype(f32)


def softmax(queries, keys, bias):
    scores = nt(queries, keys) * SCALE + bias
    weights = jnp.exp(scores - jnp.max(scores, axis=-1, keepdims=True))
    return (weights / jnp.sum(weights, axis=-1, keepdims=True)).astype(bf16)


def lay(pieces, at, width, rows_ref):
    share = pieces[0].shape[0]
    for k, piece in enumerate(pieces):
        rows_ref[k * share : (k + 1) * share, :] = piece[:, at : at + width]


def forward_body(here, docs, p0, p1, p2, p3, w_q, w_k, w_v, w_o, o0, o1, o2, o3, rows):
    width = rows.shape[1]
    lay((p0, p1, p2, p3), 0, width, rows)
    bias = bias_of(here[0], docs[0:1, :], p0.shape[0] // 4)
    queries = nn(rows[...], w_q[...]).astype(bf16)
    keys = nn(rows[...], w_k[...]).astype(bf16)
    values = nn(rows[...], w_v[...]).astype(bf16)
    mixed = [
        nn(softmax(queries[:, h : h + HEAD], keys, bias), values).astype(bf16)
        for h in range(0, queries.shape[1], HEAD)
    ]
    mixed = jnp.concatenate(mixed, axis=1)
    for c in range(0, width, STRIPE):
        term = nt(mixed, w_o[c : c + STRIPE, :]).astype(bf16)
        share = o0.shape[0]
        for k, out in enumerate((o0, o1, o2, o3)):
            out[:, c : c + STRIPE] = term[k * share : (k + 1) * share]


def backward_body(
    here, docs, p0, p1, p2, p3, w_q, w_k, w_v, w_o, o0, o1, o2, o3, exchange, rows, grads
):
    width = rows.shape[1]
    lay((p0, p1, p2, p3), 0, width, rows)
    lay((p0, p1, p2, p3), width, width, grads)
    bias = bias_of(here[0], docs[1:2, :], p0.shape[0] // 4)
    queries = nn(rows[...], w_q[...]).astype(bf16)
    keys = nn(rows[...], w_k[...]).astype(bf16)
    values = nn(rows[...], w_v[...]).astype(bf16)
    dmixed = nn(grads[...], w_o[...]).astype(bf16)
    dqueries, dkeys, dvalues = [], 0.0, 0.0
    for h in range(0, queries.shape[1], HEAD):
        q, dm = queries[:, h : h + HEAD], dmixed[:, h : h + HEAD]
        probs = softmax(q, keys, bias)
        wide = probs.astype(f32)
        dprobs = nt(dm, values)
        inner = jnp.sum(wide * dprobs, axis=-1, keepdims=True)
        dscores = (wide * (dprobs - inner) * SCALE).astype(bf16)
        dqueries.append(nn(dscores, keys).astype(bf16))
        dkeys = dkeys + tn(dscores, q)
        dvalues = dvalues + tn(probs, dm)
    dqueries = jnp.concatenate(dqueries, axis=1)
    dkeys, dvalues = dkeys.astype(bf16), dvalues.astype(bf16)
    for c in range(0, width, STRIPE):
        at = slice(c, c + STRIPE)
        term = nt(dqueries, w_q[at, :]) + nt(dkeys, w_k[at, :]) + nt(dvalues, w_v[at, :])
        term = term.astype(bf16)
        share = o0.shape[0]
        for k, out in enumerate((o0, o1, o2, o3)):
            out[:, at] = term[k * share : (k + 1) * share]
    columns = jnp.concatenate([dqueries, dkeys, dvalues], axis=1)
    part = exchange.shape[2] - columns.shape[1]
    for c in range(exchange.shape[0]):
        exchange[c, :, :part] = rows[:, c * part : (c + 1) * part]
        exchange[c, :, part:] = columns


def half_body(here, a0, a1, a2, a3, o0, o1, o2, o3):
    count = a0.shape[0]
    for k, out in enumerate((o0, o1, o2, o3)):
        at = lax.rem(here[0] + k, count)
        total = a0[at].astype(f32) + a1[at].astype(f32) + a2[at].astype(f32) + a3[at].astype(f32)
        out[...] = total.astype(bf16)


def back_tail(a0, a1, a2, a3, stash, grad, out):
    dnormed = sum(ref[...].astype(f32) for ref in (a0, a1, a2, a3))
    scaled, inverse = unit(stash[...])
    slope = jnp.mean(dnormed * scaled, axis=-1, keepdims=True)
    out[...] = (grad[...].astype(f32) + inverse * (dnormed - scaled * slope)).astype(bf16)


def ahead_tail(a0, a1, a2, a3, act, out):
    attended = sum(ref[...].astype(f32) for ref in (a0, a1, a2, a3))
    out[...] = (act[...].astype(f32) + attended).astype(bf16)


def weights_body(exchange, g_q, g_k, g_v):
    part, nq, nk = g_q.shape[0], g_q.shape[1], g_k.shape[1]
    for out, at in ((g_q, 0), (g_k, nq), (g_v, nq + nk)):
        total = 0.0
        for c in range(exchange.shape[0]):
            columns = exchange[c, :, part + at : part + at + out.shape[1]]
            total = total + tn(exchange[c, :, :part], columns)
        out[...] = total


def collect(block, axis):
    count = lax.axis_size(axis)
    steps = sorted(range(1, count), key=lambda k: min(k, count - k))
    found = {step: shift(block, axis, -step) for step in steps}
    return [block] + [found[step] for step in range(1, count)]


def deal(blocks, axis):
    count = lax.axis_size(axis)
    steps = sorted(range(1, count), key=lambda k: min(k, count - k))
    return [blocks[0]] + [shift(blocks[step], axis, step) for step in steps]


def body(act_in, stash_in, grad_in, doc_ids, query_weight, key_weight, value_weight, out_weight):
    nz, nx, nd = lax.axis_size("tz"), lax.axis_size("tx"), lax.axis_size("dp")
    act, stash, grad = act_in[0, 0], stash_in[0, 0], grad_in[0, 0]
    matrices = (query_weight[0], key_weight[0], value_weight[0], out_weight[0])
    nq, nk = query_weight.shape[2], key_weight.shape[2]
    share, width = act.shape
    seq = share * nz * nx
    place = lax.axis_index("tz").astype(jnp.int32).reshape(1)
    here = lax.axis_index("tx").astype(jnp.int32).reshape(1)
    docs = doc_ids[0, 0]

    tall = pltpu.VMEM((seq, width), bf16)
    piece = struct((seq // nx, width))

    def halves(pieces):
        cut = [p.reshape(nz, share, width) for p in pieces]
        return kernel(half_body, [struct((share, width))] * nz, [], place, *cut, flops=1 << 22)

    mine = struct((share, 3 * width))
    mine = kernel(norm_body, mine, [], stash, grad, act, flops=1 << 22, room=8)
    by_z = lax.all_gather(mine, "tz", axis=0, tiled=True)
    behind, ahead = by_z[:, : 2 * width], by_z[:, 2 * width :]
    behind = collect(behind, "tx")
    ahead = collect(ahead, "tx")

    *partial, exchange = kernel(
        backward_body,
        [piece] * nx + [struct((nd, seq, width // nd + nq + 2 * nk))],
        [tall, tall],
        here, docs, *behind, *matrices,
        flops=2 * seq * width * (3 * nq + 4 * nk),
    )
    exchange = swap(exchange, "dp")
    partial = deal(partial, "tx")
    partial = halves(partial)
    partial = deal(partial, "tz")
    grad_back = kernel(back_tail, struct((share, width)), [], *partial, stash, grad, room=8)
    grad_out = shift(grad_back, "pp", -1)

    partial = kernel(
        forward_body,
        [piece] * nx,
        [tall],
        here, docs, *ahead, *matrices,
        flops=2 * seq * width * (2 * nq + 2 * nk),
    )
    partial = deal(partial, "tx")
    partial = halves(partial)
    partial = deal(partial, "tz")
    outgoing = kernel(ahead_tail, struct((share, width)), [], *partial, act, room=8)
    act_out = shift(outgoing, "pp", 1)

    part = width // nd
    grads = kernel(
        weights_body,
        [struct((part, n), f32) for n in (nq, nk, nk)],
        [],
        exchange,
        flops=2 * nd * seq * part * (nq + 2 * nk),
    )
    return (act_out[None, None], grad_out[None, None], *(g[None] for g in grads))


def solution(mesh):
    sizes = dict(mesh.shape)
    nz = 4
    grid = mesh.devices.reshape(sizes["pp"], nz, sizes["tp"] // nz, sizes["dp"])
    split = Mesh(grid, ("pp", "tz", "tx", "dp"))
    rows = P("pp", "dp", ("tz", "tx"), None)
    cols = P("pp", None, ("tz", "tx"))
    grads = P("pp", "dp", ("tz", "tx"))
    return jax.shard_map(
        body,
        mesh=split,
        in_specs=(rows, rows, rows, P("pp", "dp", None, None), cols, cols, cols, cols),
        out_specs=(rows, rows, grads, grads, grads),
        check_vma=False,
    )
```

```python
import math

import jax
import jax.numpy as jnp
from jax import lax
from jax.experimental import pallas as pl
from jax.experimental.pallas import tpu as pltpu
from jax.sharding import Mesh, PartitionSpec as P


HEAD = 128
SCALE = 1.0 / math.sqrt(HEAD)
STRIPE = 512
epsilon = 1e-05
bf16 = jnp.bfloat16
f32 = jnp.float32


def shift(value, axis, steps):
    count = lax.axis_size(axis)
    return lax.ppermute(value, axis, [(i, (i + steps) % count) for i in range(count)])


def dot(a, b, left, right):
    return lax.dot_general(a, b, (((left,), (right,)), ((), ())), preferred_element_type=f32)


def nn(a, b):
    return dot(a, b, 1, 0)


def nt(a, b):
    return dot(a, b, 1, 1)


def tn(a, b):
    return dot(a, b, 0, 0)


def kernel(fn, out, scratch, *args, flops=0, room=16, space=pltpu.VMEM):
    taken, vmem = pl.BlockSpec(memory_space=space), pl.BlockSpec(memory_space=pltpu.VMEM)
    smem = pl.BlockSpec(memory_space=pltpu.SMEM)
    size = sum(a.size * a.dtype.itemsize for a in args)
    return pl.pallas_call(
        fn,
        out_shape=out,
        in_specs=[smem if a.shape == (1,) else taken for a in args],
        out_specs=jax.tree.map(lambda _: vmem, out),
        scratch_shapes=scratch,
        compiler_params=pltpu.CompilerParams(vmem_limit_bytes=room << 20),
        cost_estimate=pl.CostEstimate(flops=flops, bytes_accessed=size, transcendentals=0),
    )(*args)


def struct(shape, dtype=bf16):
    return jax.ShapeDtypeStruct(shape, dtype)


def unit(rows):
    wide = rows.astype(f32)
    inverse = lax.rsqrt(jnp.mean(wide * wide, axis=-1, keepdims=True) + epsilon)
    return wide * inverse, inverse


def norm_body(stash, grad, act, out, held, sems):
    width = act.shape[1]
    copies = [
        pltpu.make_async_copy(ref, held.at[k], sems.at[k])
        for k, ref in enumerate((stash, act))
    ]
    copies.append(pltpu.make_async_copy(grad, held.at[2], sems.at[2]))
    for copy in copies:
        copy.start()
    for k, at in enumerate((0, 2)):
        copies[k].wait()
        out[:, at * width : (at + 1) * width] = unit(held[k])[0].astype(bf16)
    copies[2].wait()
    out[:, width : 2 * width] = held[2]


def bias_of(here, docs, share):
    seq = docs.shape[1]
    count = 4
    wide = seq // count

    def position(axis):
        row = lax.broadcasted_iota(jnp.int32, (seq, seq), axis)
        step = row // wide
        at_x = lax.rem(here + step, count)
        at_z = (row - step * wide) // share
        return (at_z * count + at_x) * share + lax.rem(row, share)

    pick = (lax.broadcasted_iota(jnp.int32, (seq, seq), 1) == position(0)).astype(f32)
    lined = jnp.broadcast_to(docs.astype(f32), (8, seq))
    down = nt(pick, lined)[:, :1]
    along = nt(lined, pick)[:1, :]
    return jnp.where((position(1) <= position(0)) & (down == along), 0.0, -jnp.inf).astype(f32)


def softmax(queries, keys, bias):
    scores = nt(queries, keys) * SCALE + bias
    weights = jnp.exp(scores - jnp.max(scores, axis=-1, keepdims=True))
    return (weights / jnp.sum(weights, axis=-1, keepdims=True)).astype(bf16)


def fetch_body(*refs):
    count = (len(refs) - 1) // 2
    copies = []
    for k in range(count):
        rows = refs[k].shape[0] // 4
        for part in range(4):
            at = pl.ds(part * rows, rows)
            copies.append(
                pltpu.make_async_copy(
                    refs[k].at[at], refs[count + k].at[at], refs[-1].at[4 * k + part]
                )
            )
    for copy in copies:
        copy.start()
    for copy in copies:
        copy.wait()


def lay(pieces, at, width, rows_ref):
    share = pieces[0].shape[0]
    for k, piece in enumerate(pieces):
        rows_ref[k * share : (k + 1) * share, :] = piece[:, at : at + width]


def run_forward(bias, queries, keys, values, w_o, outs):
    width = w_o.shape[0]
    mixed = [
        nn(softmax(queries[:, h : h + HEAD], keys, bias), values).astype(bf16)
        for h in range(0, queries.shape[1], HEAD)
    ]
    mixed = jnp.concatenate(mixed, axis=1)
    for c in range(0, width, STRIPE):
        term = nt(mixed, w_o[c : c + STRIPE, :]).astype(bf16)
        share = outs[0].shape[0]
        for k, out in enumerate(outs):
            out[:, width + c : width + c + STRIPE] = term[k * share : (k + 1) * share]


def run_backward(bias, queries, keys, values, dmixed, w_q, w_k, w_v, outs):
    width = w_q.shape[0]
    dqueries, dkeys, dvalues = [], 0.0, 0.0
    for h in range(0, queries.shape[1], HEAD):
        q, dm = queries[:, h : h + HEAD], dmixed[:, h : h + HEAD]
        probs = softmax(q, keys, bias)
        wide = probs.astype(f32)
        dprobs = nt(dm, values)
        inner = jnp.sum(wide * dprobs, axis=-1, keepdims=True)
        dscores = (wide * (dprobs - inner) * SCALE).astype(bf16)
        dqueries.append(nn(dscores, keys).astype(bf16))
        dkeys = dkeys + tn(dscores, q)
        dvalues = dvalues + tn(probs, dm)
    dqueries = jnp.concatenate(dqueries, axis=1)
    dkeys, dvalues = dkeys.astype(bf16), dvalues.astype(bf16)
    for c in range(0, width, STRIPE):
        at = slice(c, c + STRIPE)
        term = nt(dqueries, w_q[at, :]) + nt(dkeys, w_k[at, :]) + nt(dvalues, w_v[at, :])
        term = term.astype(bf16)
        share = outs[0].shape[0]
        for k, out in enumerate(outs):
            out[:, at] = term[k * share : (k + 1) * share]
    return jnp.concatenate([dqueries, dkeys, dvalues], axis=1)


def both_body(here, docs, *refs):
    pieces, (w_q, w_k, w_v, w_o), outs = refs[:4], refs[4:8], refs[8:12]
    behind, columns, ahead, grads = refs[12:]
    width, share = grads.shape[1], pieces[0].shape[0] // 4
    lay(pieces, 0, width, behind)
    lay(pieces, width, width, grads)
    queries, keys, values = (nn(behind[...], w[...]).astype(bf16) for w in (w_q, w_k, w_v))
    dmixed = nn(grads[...], w_o[...]).astype(bf16)
    bias = bias_of(here[0], docs[1:2, :], share)
    columns[...] = run_backward(bias, queries, keys, values, dmixed, w_q, w_k, w_v, outs)
    lay(pieces, 2 * width, width, ahead)
    queries, keys, values = (nn(ahead[...], w[...]).astype(bf16) for w in (w_q, w_k, w_v))
    run_forward(bias_of(here[0], docs[0:1, :], share), queries, keys, values, w_o, outs)


def parcel_body(copy, behind, columns, *sent):
    part = behind.shape[1] // len(sent)
    for k, out in enumerate(sent):
        at = lax.rem(copy[0] + k, len(sent)) * part
        out[:, :part] = behind[:, pl.ds(pl.multiple_of(at, part), part)]
        out[:, part:] = columns[...]


def half_body(place, a0, a1, a2, a3, keep_b, send_b, keep_f, send_f):
    width = keep_b.shape[2]
    own, last = place[0], a0.shape[0] - 1
    beside = own + 1 - 2 * lax.rem(own, 2)
    plan = (
        (keep_b, 0, (own, last - own)),
        (send_b, 0, (beside, last - beside)),
        (keep_f, width, (own, beside)),
        (send_f, width, (last - own, last - beside)),
    )
    for out, at, chunks in plan:
        for k, chunk in enumerate(chunks):
            total = sum(a[chunk, :, at : at + width].astype(f32) for a in (a0, a1, a2, a3))
            out[k] = total.astype(bf16)


def through_norm(dnormed, scaled, inverse):
    return inverse * (dnormed - scaled * jnp.mean(dnormed * scaled, axis=-1, keepdims=True))


def join_back(keep, came, stash, beside, grad, own, other):
    first = through_norm(keep[0].astype(f32) + came[0].astype(f32), *unit(stash[...]))
    own[...] = (grad[...].astype(f32) + first).astype(bf16)
    second = through_norm(keep[1].astype(f32) + came[1].astype(f32), *unit(beside[...]))
    other[...] = second.astype(bf16)


def join_ahead(keep, came, act, own, other):
    own[...] = (act[...].astype(f32) + keep[0].astype(f32) + came[0].astype(f32)).astype(bf16)
    other[...] = (keep[1].astype(f32) + came[1].astype(f32)).astype(bf16)


def end_body(own, other, out):
    out[...] = (own[...].astype(f32) + other[...].astype(f32)).astype(bf16)


def weights_body(*refs):
    sent, (g_q, g_k, g_v) = refs[:-3], refs[-3:]
    part, nq, nk = g_q.shape[0], g_q.shape[1], g_k.shape[1]
    for out, at in ((g_q, 0), (g_k, nq), (g_v, nq + nk)):
        total = 0.0
        for one in sent:
            total = total + tn(one[:, :part], one[:, part + at : part + at + out.shape[1]])
        out[...] = total


def across(value, axis, mask):
    count = lax.axis_size(axis)
    return lax.ppermute(value, axis, [(i, i ^ mask) for i in range(count)])


def collect(block, axis):
    count = lax.axis_size(axis)
    steps = sorted(range(1, count), key=lambda k: min(k, count - k))
    found = {step: shift(block, axis, -step) for step in steps}
    return [block] + [found[step] for step in range(1, count)]


def slant(value, steps, mask):
    np, nz = lax.axis_size("pp"), lax.axis_size("tz")
    pairs = [
        (p * nz + z, (p + steps) % np * nz + (z ^ mask)) for p in range(np) for z in range(nz)
    ]
    return lax.ppermute(value, ("pp", "tz"), pairs)


def deal(blocks, axis):
    count = lax.axis_size(axis)
    steps = sorted(range(1, count), key=lambda k: min(k, count - k))
    return [blocks[0]] + [shift(blocks[step], axis, step) for step in steps]


def body(act_in, stash_in, grad_in, doc_ids, query_weight, key_weight, value_weight, out_weight):
    nz, nx, nd = lax.axis_size("tz"), lax.axis_size("tx"), lax.axis_size("dp")
    act, stash, grad = act_in[0, 0], stash_in[0, 0], grad_in[0, 0]
    matrices = (query_weight[0], key_weight[0], value_weight[0], out_weight[0])
    nq, nk = query_weight.shape[2], key_weight.shape[2]
    share, width = act.shape
    seq, part = share * nz * nx, width // nd
    here, place, copy = (
        lax.axis_index(axis).astype(jnp.int32).reshape(1) for axis in ("tx", "tz", "dp")
    )

    mine = kernel(
        norm_body,
        struct((share, 3 * width)),
        [pltpu.VMEM((3, share, width), bf16), pltpu.SemaphoreType.DMA((3,))],
        stash, grad, act,
        flops=1 << 22, room=8, space=pltpu.HBM,
    )
    by_z = lax.all_gather(mine, "tz", axis=0, tiled=True)
    pieces = collect(by_z, "tx")
    beside = across(stash, "tz", nz - 1)
    matrices = kernel(
        fetch_body,
        [struct(m.shape) for m in matrices],
        [pltpu.SemaphoreType.DMA((16,))],
        *matrices,
        flops=1 << 22, room=4, space=pltpu.HBM,
    )
    tall = pltpu.VMEM((seq, width), bf16)
    outs = [struct((seq // nx, 2 * width))] * nx
    *partial, behind, columns = kernel(
        both_body,
        outs + [struct((seq, width)), struct((seq, nq + 2 * nk))],
        [tall, tall],
        here, doc_ids[0, 0], *pieces, *matrices,
        flops=2 * seq * width * (5 * nq + 6 * nk), room=24,
    )
    partial = deal(partial, "tx")
    parcels = kernel(
        parcel_body, [struct((seq, part + nq + 2 * nk))] * nd, [],
        copy, behind, columns, flops=1 << 22, room=4,
    )
    far = sorted(range(1, nd), key=lambda k: -min(k, nd - k))
    sent = [parcels[0]]
    for steps in (far[:4], far[4:]):
        sent += [shift(parcels[step], "dp", step) for step in steps]
    pair = struct((2, share, width))
    partial = [p.reshape(nz, share, 2 * width) for p in partial]
    keep_b, send_b, keep_f, send_f = kernel(
        half_body, [pair] * 4, [], place, *partial, flops=1 << 23, room=8
    )
    came_b = across(send_b, "tz", 1)
    came_f = across(send_f, "tz", nz - 1)
    row = struct((share, width))
    own_b, other_b = kernel(
        join_back, [row, row], [], keep_b, came_b, stash, beside, grad, flops=1 << 20, room=4
    )
    other_b, own_b = slant(other_b, -1, nz - 1), shift(own_b, "pp", -1)
    own_f, other_f = kernel(join_ahead, [row, row], [], keep_f, came_f, act, flops=1 << 20, room=4)
    other_f, own_f = slant(other_f, 1, 1), shift(own_f, "pp", 1)
    grad_out = kernel(end_body, row, [], own_b, other_b, flops=1 << 20, room=4)[None, None]
    act_out = kernel(end_body, row, [], own_f, other_f, flops=1 << 20, room=4)[None, None]
    grads = kernel(
        weights_body,
        [struct((part, n), f32) for n in (nq, nk, nk)],
        [],
        *sent,
        flops=2 * nd * seq * part * (nq + 2 * nk),
    )
    return (act_out, grad_out, *(g[None] for g in grads))


def solution(mesh):
    sizes = dict(mesh.shape)
    nz = 4
    grid = mesh.devices.reshape(sizes["pp"], nz, sizes["tp"] // nz, sizes["dp"])
    split = Mesh(grid, ("pp", "tz", "tx", "dp"))
    rows = P("pp", "dp", ("tz", "tx"), None)
    cols = P("pp", None, ("tz", "tx"))
    grads = P("pp", "dp", ("tz", "tx"))
    return jax.shard_map(
        body,
        mesh=split,
        in_specs=(rows, rows, rows, P("pp", "dp", None, None), cols, cols, cols, cols),
        out_specs=(rows, rows, grads, grads, grads),
        check_vma=False,
    )
```
